32 devices in a mesh: group: 2 (over x), ctx: 8 (over z, y), tp: 2 (over core).
Axes of the slice: x: 2, y: 2, z: 4, core: 2. Of those that a mesh axis runs over, the one named last changes fastest.
Arguments:
- stretch_query: bfloat16 [2, 1024, 8192], P('group', 'ctx', 'tp'), may hold values from -8 to 8
- prefix_keyvals: bfloat16 [2, 2, 8192, 1024], P('group', None, 'ctx', 'tp'), may hold values from -6 to 6
- stretch_key_values: bfloat16 [2, 2, 1024, 1024], P('group', None, 'ctx', 'tp'), may hold values from -6 to 6
- stretch_start: int32 [2], P('group'), may hold values from 2048 to 8192
- decode_query: bfloat16 [256, 4, 8192], P(('group', 'ctx'), None, 'tp'), may hold values from -8 to 8
- draft_key_values: bfloat16 [2, 256, 4, 1024], P(None, ('group', 'ctx'), None, 'tp'), may hold values from -6 to 6
- decode_cache: bfloat16 [2, 256, 1024, 1024], P(None, ('group', 'ctx'), None, 'tp'), may hold values from -6 to 6
- cache_lengths: int32 [256], P(('group', 'ctx')), may hold values from 128 to 1024, as said below
- page_rows: int32 [16], replicated, may hold values from 0 to 255, as said below
Outputs:
- prefill_out: bfloat16 [2, 1024, 8192], P('group', 'ctx', 'tp')
- decode_out: bfloat16 [256, 4, 8192], P(('group', 'ctx'), None, 'tp')
The draws below stay inside these ranges and needn't reach their ends.
Inputs may be any that keep to these rules, and one draw needn't show every extreme that they name: `cache_lengths`: one row has length 1024. `page_rows`: page n = g * 8 + c names one of the rows m * 16 to m * 16 + 15, where m = (n + 1) mod 16 if n mod 4 = 1, m = g * 8 + (c + 8 / 2) mod 8 if n mod 4 = 3, and m = (n + 8) mod 16 for even n; no row is named twice.
All inputs are finite; a program needn't handle non-finite values.
Results may differ from the reference program's by a relative error of at most 0.0049.
Values may be sent and summed in bfloat16 or wider, within the bound.
A program may use at most 128 MiB of HBM per device.

```python
import math
import jax
import jax.numpy as jnp
from jax import lax

QUERY_HEADS = 64
KEY_VALUE_HEADS = 8
HEAD_SIZE = 128
STRETCH_DEV = 128
ROWS_DEV = 16
ROW_CACHE_LIMIT = 1024
DRAFT_TOKENS = 4
QUERY_GROUP = 8
PREFILL_COUNT = 2
STRETCH_LENGTH = 1024
PREFIX_LENGTH = 8192
DECODE_ROWS = 256
PAGES = 16
N_CTX = 8


def draw_stretch_query(key, part):
    local = jax.random.fold_in(key, 11)
    values = jnp.clip(2.5 * jax.random.normal(local, (PREFILL_COUNT, STRETCH_LENGTH, QUERY_HEADS * HEAD_SIZE), jnp.float32), -8.0, 8.0)
    return values.astype(jnp.bfloat16)


def draw_prefix_keyvals(key, part):
    local = jax.random.fold_in(key, 21)
    array_shape = (PREFILL_COUNT, 2, PREFIX_LENGTH, KEY_VALUE_HEADS * HEAD_SIZE)
    values = jnp.clip(jax.random.normal(local, array_shape, jnp.float32), -6.0, 6.0)
    return values.astype(jnp.bfloat16)


def draw_decode_query(key, part):
    local = jax.random.fold_in(key, 31)
    array_shape = (DECODE_ROWS, DRAFT_TOKENS, QUERY_HEADS * HEAD_SIZE)
    values = jnp.clip(2.5 * jax.random.normal(local, array_shape, jnp.float32), -8.0, 8.0)
    return values.astype(jnp.bfloat16)


def draw_decode_cache(key, part):
    local = jax.random.fold_in(key, 41)
    array_shape = (2, DECODE_ROWS, ROW_CACHE_LIMIT, KEY_VALUE_HEADS * HEAD_SIZE)
    values = jnp.clip(jax.random.normal(local, array_shape, jnp.float32), -6.0, 6.0)
    return values.astype(jnp.bfloat16)


def draw_cache_lengths(key, part):
    blocks = DECODE_ROWS // ROWS_DEV
    levels = (ROW_CACHE_LIMIT // STRETCH_DEV).bit_length() - 1
    power = jax.random.randint(jax.random.fold_in(key, 51), (blocks, 1), 0, levels + 1)
    ceiling = STRETCH_DEV * 2 ** power
    spread = jax.random.randint(jax.random.fold_in(key, 52), (blocks, ROWS_DEV), 0, ceiling - STRETCH_DEV + 1)
    lengths = (STRETCH_DEV + spread).reshape(DECODE_ROWS)
    longest = jax.random.randint(jax.random.fold_in(key, 53), (), 0, DECODE_ROWS)
    lengths = jnp.where(jnp.arange(DECODE_ROWS) == longest, ROW_CACHE_LIMIT, lengths)
    return lengths.astype(jnp.int32)


def draw_page_rows(key, part):
    page_ids = jnp.arange(PAGES, dtype=jnp.int32)
    kind = page_ids % 4
    odd_page = page_ids % 2 == 1
    position = page_ids % N_CTX
    half_away = page_ids - position + (position + N_CTX // 2) % N_CTX
    target_block = jnp.where(kind == 1, page_ids + 1, jnp.where(kind == 3, half_away, page_ids + PAGES // 2)) % PAGES
    first_row = jax.random.randint(jax.random.fold_in(key, 61), (PAGES,), 0, ROWS_DEV)
    second_row = (first_row + 1 + jax.random.randint(jax.random.fold_in(key, 62), (PAGES,), 0, ROWS_DEV - 1)) % ROWS_DEV
    within = jnp.where(odd_page, first_row[target_block], second_row[target_block])
    return (target_block * ROWS_DEV + within).astype(jnp.int32)


def level_of(stream_key, shape, pieces, low, largest):
    loudness = 1.0
    for axis_at, shards_of in pieces:
        steps = jax.random.uniform(jax.random.fold_in(jax.random.fold_in(stream_key, 6), axis_at), (shards_of,), jnp.float32, low / len(pieces), largest / len(pieces))
        loudness = loudness * jnp.repeat(jnp.exp(steps), shape[axis_at] // shards_of).reshape((-1,) + (1,) * (len(shape) - 1 - axis_at))
    return loudness


def gaussian(own_key, dims, scale, most, split=(), kind=jnp.bfloat16):
    gain = level_of(own_key, dims, split, -0.22, 0.18) if split else 1.0
    drawn = jax.random.normal(own_key, dims, jnp.float32) * scale * gain
    return jnp.minimum(jnp.maximum(drawn, -most), most).astype(kind)


def setup_inputs(seed: int = 0) -> dict:
    streams_of = jax.random.split(jax.random.key(seed), 10)
    stretch_query = draw_stretch_query(jax.random.fold_in(streams_of[9], 71), 0)
    prefix_keyvals = draw_prefix_keyvals(jax.random.fold_in(streams_of[9], 71), 0)
    stretch_key_values = gaussian(streams_of[2], (PREFILL_COUNT, 2, STRETCH_LENGTH, KEY_VALUE_HEADS * HEAD_SIZE), 1.0, 6.0, ((0, 2), (2, 8), (3, 2)))
    stretch_start = jax.random.randint(streams_of[3], (PREFILL_COUNT,), PREFIX_LENGTH // 4, PREFIX_LENGTH + 1).astype(jnp.int32)
    decode_query = draw_decode_query(jax.random.fold_in(streams_of[9], 71), 0)
    draft_key_values = gaussian(streams_of[5], (2, DECODE_ROWS, DRAFT_TOKENS, KEY_VALUE_HEADS * HEAD_SIZE), 1.0, 6.0, ((1, 16), (3, 2)))
    decode_cache = draw_decode_cache(jax.random.fold_in(streams_of[9], 71), 0)
    cache_lengths = draw_cache_lengths(jax.random.fold_in(streams_of[9], 71), 0)
    page_rows = draw_page_rows(jax.random.fold_in(streams_of[9], 71), 0)
    return dict(stretch_query=stretch_query, prefix_keyvals=prefix_keyvals, stretch_key_values=stretch_key_values, stretch_start=stretch_start, decode_query=decode_query, draft_key_values=draft_key_values, decode_cache=decode_cache, cache_lengths=cache_lengths, page_rows=page_rows)


def attend_rows(queries, rows_of_keys, rows_of_values, allowed):
    scores = jnp.dot(queries, rows_of_keys.T, preferred_element_type=jnp.float32) * (1.0 / math.sqrt(HEAD_SIZE))
    masked = jnp.where(allowed, scores, -jnp.inf)
    highest = lax.optimization_barrier(jnp.max(masked, axis=-1, keepdims=True))
    weights = jnp.exp(masked - highest)
    totals = lax.optimization_barrier(jnp.sum(weights, axis=-1, keepdims=True))
    summed = jnp.dot(weights.astype(jnp.bfloat16), rows_of_values, preferred_element_type=jnp.float32)
    return (summed / totals).astype(jnp.bfloat16)

def prefill_request(query, prefix_length, stretch_length, limit):
    total_length = PREFIX_LENGTH + STRETCH_LENGTH
    heads_q = query.reshape(STRETCH_LENGTH, QUERY_HEADS, HEAD_SIZE).transpose(1, 0, 2)
    joined_keys = jnp.concatenate([prefix_length[0], stretch_length[0]], axis=0).reshape(total_length, KEY_VALUE_HEADS, HEAD_SIZE).transpose(1, 0, 2)
    joined_values = jnp.concatenate([prefix_length[1], stretch_length[1]], axis=0).reshape(total_length, KEY_VALUE_HEADS, HEAD_SIZE).transpose(1, 0, 2)
    key_pos = jnp.arange(total_length, dtype=jnp.int32)
    query_pos = jnp.arange(STRETCH_LENGTH, dtype=jnp.int32)
    allowed = jnp.where(key_pos[None, :] < PREFIX_LENGTH, key_pos[None, :] < limit, (key_pos - PREFIX_LENGTH)[None, :] <= query_pos[:, None])

    def one_head(head_index):
        kv_index = head_index // QUERY_GROUP
        return attend_rows(heads_q[head_index], joined_keys[kv_index], joined_values[kv_index], allowed)
    result = lax.map(one_head, jnp.arange(QUERY_HEADS, dtype=jnp.int32))
    return result.transpose(1, 0, 2).reshape(STRETCH_LENGTH, QUERY_HEADS * HEAD_SIZE)

def reference(stretch_query, prefix_keyvals, stretch_key_values, stretch_start, decode_query, draft_key_values, decode_cache, cache_lengths, page_rows):
    results = []
    for request in range(PREFILL_COUNT):
        results.append(prefill_request(stretch_query[request], prefix_keyvals[request], stretch_key_values[request], stretch_start[request]))
    prefill_out = jnp.stack(results)
    column_count = KEY_VALUE_HEADS * HEAD_SIZE
    pages = stretch_key_values.reshape(PREFILL_COUNT, 2, N_CTX, STRETCH_DEV, column_count).transpose(0, 2, 1, 3, 4).reshape(PAGES, 2, STRETCH_DEV, column_count)
    token_span = ROW_CACHE_LIMIT + DRAFT_TOKENS
    key_pos = jnp.arange(token_span, dtype=jnp.int32)
    step_pos = jnp.arange(DRAFT_TOKENS, dtype=jnp.int32)

    def one_row(row_index):
        matches = page_rows == row_index
        has_page = jnp.any(matches)
        page_block = jnp.einsum('p,pcsd->csd', matches.astype(jnp.float32), pages.astype(jnp.float32)).astype(jnp.bfloat16)
        row_cache = decode_cache[:, row_index]
        head_part = jnp.where(has_page, page_block, row_cache[:, :STRETCH_DEV])
        fresh = draft_key_values[:, row_index]
        rows_of_keys = jnp.concatenate([head_part[0], row_cache[0, STRETCH_DEV:], fresh[0]], axis=0)
        rows_of_values = jnp.concatenate([head_part[1], row_cache[1, STRETCH_DEV:], fresh[1]], axis=0)
        heads_of_keys = jnp.repeat(rows_of_keys.reshape(token_span, KEY_VALUE_HEADS, HEAD_SIZE).transpose(1, 0, 2), QUERY_GROUP, axis=0)
        heads_of_values = jnp.repeat(rows_of_values.reshape(token_span, KEY_VALUE_HEADS, HEAD_SIZE).transpose(1, 0, 2), QUERY_GROUP, axis=0)
        allowed = jnp.where(key_pos[None, :] < ROW_CACHE_LIMIT, key_pos[None, :] < cache_lengths[row_index], (key_pos - ROW_CACHE_LIMIT)[None, :] <= step_pos[:, None])
        heads_q = decode_query[row_index].reshape(DRAFT_TOKENS, QUERY_HEADS, HEAD_SIZE).transpose(1, 0, 2)
        result = jax.vmap(attend_rows, in_axes=(0, 0, 0, None))(heads_q, heads_of_keys, heads_of_values, allowed)
        return result.transpose(1, 0, 2).reshape(DRAFT_TOKENS, QUERY_HEADS * HEAD_SIZE)
    decode_out = lax.map(one_row, jnp.arange(DECODE_ROWS, dtype=jnp.int32))
    return (prefill_out, decode_out)
```

```python
import functools
import math

import jax
import jax.numpy as jnp
from jax import lax
from jax.experimental import pallas as pl
from jax.experimental.pallas import tpu as pltpu
from jax.sharding import PartitionSpec as P

QUERY_HEADS = 64
KEY_VALUE_HEADS = 8
HEAD_SIZE = 128
QUERY_GROUP = QUERY_HEADS // KEY_VALUE_HEADS
SCALE2 = math.log2(math.e) / math.sqrt(HEAD_SIZE)
LOW = -1e30


def nt(a, b):
    return lax.dot_general(a, b, (((1,), (1,)), ((), ())), preferred_element_type=jnp.float32)


def tn(a, b):
    return lax.dot_general(a, b, (((0,), (0,)), ((), ())), preferred_element_type=jnp.float32)


def decode_kernel(
    heads, steps, page_size, info, q_ref, cache_ref, draft_ref, even_ref, odd_ref, out_ref, wide
):
    row = pl.program_id(0)
    length = info[row]
    rows_per_head = QUERY_GROUP * steps
    lanes = heads * rows_per_head

    @pl.when(row == 0)
    def _():
        wide[...] = jnp.zeros_like(wide)

    for h in range(heads):
        wide[h * rows_per_head : (h + 1) * rows_per_head, h * HEAD_SIZE : (h + 1) * HEAD_SIZE] = (
            q_ref[0, h]
        )
    queries = wide[...]
    row_count = pl.num_programs(0)
    is_even = info[row_count] == row
    is_odd = info[row_count + 1] == row

    def first(part):
        here = cache_ref[part, 0, :page_size, :]
        return jnp.where(is_even, even_ref[part], jnp.where(is_odd, odd_ref[part], here))

    positions = cache_ref.shape[2]
    rest = positions - page_size
    s0 = nt(first(0), queries)
    s1 = nt(cache_ref[0, 0, page_size:, :], queries)
    s2 = nt(draft_ref[0, 0], queries)
    pos0 = lax.broadcasted_iota(jnp.int32, (page_size, lanes), 0)
    pos1 = lax.broadcasted_iota(jnp.int32, (rest, lanes), 0) + page_size
    pos2 = lax.broadcasted_iota(jnp.int32, s2.shape, 0)
    step = lax.broadcasted_iota(jnp.int32, s2.shape, 1) % steps
    s0 = jnp.where(pos0 < length, s0, -jnp.inf)
    s1 = jnp.where(pos1 < length, s1, -jnp.inf)
    s2 = jnp.where(pos2 <= step, s2, -jnp.inf)
    top = jnp.maximum(
        jnp.maximum(jnp.max(s0, axis=0, keepdims=True), jnp.max(s1, axis=0, keepdims=True)),
        jnp.max(s2, axis=0, keepdims=True),
    )
    anchor = top * SCALE2
    w0 = jnp.exp2(s0 * SCALE2 - anchor)
    w1 = jnp.exp2(s1 * SCALE2 - anchor)
    w2 = jnp.exp2(s2 * SCALE2 - anchor)
    total = (
        jnp.sum(w0, axis=0, keepdims=True)
        + jnp.sum(w1, axis=0, keepdims=True)
        + jnp.sum(w2, axis=0, keepdims=True)
    )
    summed = tn(w0.astype(jnp.bfloat16), first(1))
    summed += tn(w1.astype(jnp.bfloat16), cache_ref[1, 0, page_size:, :])
    summed += tn(w2.astype(jnp.bfloat16), draft_ref[1, 0])
    inverse = jnp.broadcast_to(1.0 / total, (8, lanes)).T[:, :1]
    summed = summed * inverse
    for h in range(heads):
        out_ref[0, h] = summed[
            h * rows_per_head : (h + 1) * rows_per_head, h * HEAD_SIZE : (h + 1) * HEAD_SIZE
        ].astype(jnp.bfloat16)


def decode(info, queries, cache, draft, even, odd, steps):
    row_count, heads, per_head, _ = queries.shape
    page_size = even.shape[1]
    columns = heads * HEAD_SIZE
    positions = cache.shape[2]
    pad = draft.shape[2]
    return pl.pallas_call(
        functools.partial(decode_kernel, heads, steps, page_size),
        grid_spec=pltpu.PrefetchScalarGridSpec(
            num_scalar_prefetch=1,
            grid=(row_count,),
            in_specs=[
                pl.BlockSpec((1, heads, per_head, HEAD_SIZE), lambda r, i: (r, 0, 0, 0)),
                pl.BlockSpec((2, 1, positions, columns), lambda r, i: (0, r, 0, 0)),
                pl.BlockSpec((2, 1, pad, columns), lambda r, i: (0, r, 0, 0)),
                pl.BlockSpec((2, page_size, columns), lambda r, i: (0, 0, 0)),
                pl.BlockSpec((2, page_size, columns), lambda r, i: (0, 0, 0)),
            ],
            out_specs=pl.BlockSpec((1, heads, per_head, HEAD_SIZE), lambda r, i: (r, 0, 0, 0)),
            scratch_shapes=[pltpu.VMEM((heads * per_head, columns), jnp.bfloat16)],
        ),
        out_shape=jax.ShapeDtypeStruct(queries.shape, jnp.bfloat16),
        cost_estimate=pl.CostEstimate(
            flops=4 * row_count * positions * columns * heads * per_head,
            bytes_accessed=cache.size * 2,
            transcendentals=row_count * positions * heads * per_head,
        ),
        name="decode_rows",
    )(info, queries, cache, draft, even, odd)


def stage_kernel(first, last, block, info, q_ref, prefix_ref, stretch_ref, *refs):
    if first:
        outs, flipped = refs[:-1], refs[-1]
    else:
        m_in, l_in, acc_in = refs[:3]
        outs, flipped = refs[3:-1], refs[-1]
    if last:
        m_ref, l_ref, own_ref, send_ref, acc_ref = outs[0], outs[1], outs[2], outs[3], refs[-2]
    else:
        m_ref, l_ref, acc_ref = outs
    limit, base, source, mine, other = info[0], info[1], info[2], info[3], info[4]
    tokens = q_ref.shape[0]
    half = tokens // 2
    keys = prefix_ref.shape[2]
    page = stretch_ref.shape[2]
    if first:
        m_ref[...] = jnp.full(m_ref.shape, LOW, jnp.float32)
        l_ref[...] = jnp.zeros(l_ref.shape, jnp.float32)
        acc_ref[...] = jnp.zeros(acc_ref.shape, jnp.float32)
    else:
        m_ref[...] = m_in[...]
        l_ref[...] = l_in[...]
        acc_ref[...] = acc_in[...]

    def absorb(key_block, turned_block, allowed):
        for g in range(QUERY_GROUP):
            q = q_ref[:, g * HEAD_SIZE : (g + 1) * HEAD_SIZE]
            scores = nt(key_block, q)
            if allowed is not None:
                scores = jnp.where(allowed, scores, -jnp.inf)
            old = m_ref[g : g + 1, :]
            new = jnp.maximum(old, jnp.max(scores, axis=0, keepdims=True))
            anchor = new * SCALE2
            weights = jnp.exp2(scores * SCALE2 - anchor)
            factor = jnp.exp2(old * SCALE2 - anchor)
            m_ref[g : g + 1, :] = new
            l_ref[g : g + 1, :] = l_ref[g : g + 1, :] * factor + jnp.sum(
                weights, axis=0, keepdims=True
            )
            product = jnp.dot(
                turned_block, weights.astype(jnp.bfloat16), preferred_element_type=jnp.float32
            )
            acc_ref[g] = acc_ref[g] * factor + product

    @pl.when(base < limit)
    def _():
        flipped[...] = prefix_ref[0, 1].T

        for at in range(0, keys, block):
            left = limit - base - at

            @pl.when(left >= block)
            def _():
                absorb(prefix_ref[0, 0, at : at + block, :], flipped[:, at : at + block], None)

            @pl.when(jnp.logical_and(left > 0, left < block))
            def _():
                allowed = lax.broadcasted_iota(jnp.int32, (block, tokens), 0) < left
                absorb(prefix_ref[0, 0, at : at + block, :], flipped[:, at : at + block], allowed)

    @pl.when(source <= jnp.maximum(mine, other))
    def _():
        lane = lax.broadcasted_iota(jnp.int32, (page, tokens), 1)
        q_pos = jnp.where(lane < half, mine * half + lane, other * half + lane - half)
        k_pos = source * page + lax.broadcasted_iota(jnp.int32, (page, tokens), 0)
        absorb(stretch_ref[0, 0], stretch_ref[0, 1].T, k_pos <= q_pos)

    if last:
        for g in range(QUERY_GROUP):
            inverse = 1.0 / l_ref[g : g + 1, :]
            done = acc_ref[g] * inverse
            own_ref[g] = done[:, :half]
            send_ref[g] = done[:, half:].astype(jnp.bfloat16)


def stage(info, queries, prefix, stretch, state, last):
    tokens = queries.shape[0]
    half = tokens // 2
    keys, columns = prefix.shape[2], prefix.shape[3]
    page = stretch.shape[2]
    heads = columns // HEAD_SIZE
    all_heads = heads * QUERY_GROUP
    first = state is None
    block = min(512, keys)
    wide = QUERY_GROUP * HEAD_SIZE
    stat_spec = pl.BlockSpec((QUERY_GROUP, tokens), lambda h, i: (h, 0))
    acc_spec = pl.BlockSpec((QUERY_GROUP, HEAD_SIZE, tokens), lambda h, i: (h, 0, 0))
    half_spec = pl.BlockSpec((QUERY_GROUP, HEAD_SIZE, half), lambda h, i: (h, 0, 0))
    in_specs = [
        pl.BlockSpec((tokens, wide), lambda h, i: (0, h)),
        pl.BlockSpec((1, 2, keys, HEAD_SIZE), lambda h, i: (0, 0, 0, h)),
        pl.BlockSpec((1, 2, page, HEAD_SIZE), lambda h, i: (0, 0, 0, h)),
    ]
    operands = [info, queries, prefix, stretch]
    if not first:
        in_specs += [stat_spec, stat_spec, acc_spec]
        operands += list(state)
    stat_shape = jax.ShapeDtypeStruct((all_heads, tokens), jnp.float32)
    scratch = [pltpu.VMEM((HEAD_SIZE, keys), jnp.bfloat16)]
    if last:
        out_specs = [stat_spec, stat_spec, half_spec, half_spec]
        out_shape = [
            stat_shape,
            stat_shape,
            jax.ShapeDtypeStruct((all_heads, HEAD_SIZE, half), jnp.float32),
            jax.ShapeDtypeStruct((all_heads, HEAD_SIZE, half), jnp.bfloat16),
        ]
        scratch = [pltpu.VMEM((QUERY_GROUP, HEAD_SIZE, tokens), jnp.float32)] + scratch
    else:
        out_specs = [stat_spec, stat_spec, acc_spec]
        out_shape = [
            stat_shape,
            stat_shape,
            jax.ShapeDtypeStruct((all_heads, HEAD_SIZE, tokens), jnp.float32),
        ]
    return pl.pallas_call(
        functools.partial(stage_kernel, first, last, block),
        grid_spec=pltpu.PrefetchScalarGridSpec(
            num_scalar_prefetch=1,
            grid=(heads,),
            in_specs=in_specs,
            out_specs=out_specs,
            scratch_shapes=scratch,
        ),
        out_shape=out_shape,
        cost_estimate=pl.CostEstimate(
            flops=6 * all_heads * tokens * (keys + page) * HEAD_SIZE,
            bytes_accessed=prefix.size * 2 + queries.size * 2,
            transcendentals=all_heads * tokens * (keys + page),
        ),
        name="prefill_stage",
    )(*operands)


def merge_kernel(own_ref, got_ref, m_ref, l_ref, m_got, l_got, out_ref):
    for g in range(QUERY_GROUP):
        ma, mb = m_ref[g : g + 1, :], m_got[g : g + 1, :]
        top = jnp.maximum(ma, mb)
        wa = l_ref[g : g + 1, :] * jnp.exp2((ma - top) * SCALE2)
        wb = l_got[g : g + 1, :] * jnp.exp2((mb - top) * SCALE2)
        inverse = 1.0 / (wa + wb)
        done = own_ref[g] * (wa * inverse) + got_ref[g].astype(jnp.float32) * (wb * inverse)
        out_ref[0, :, g * HEAD_SIZE : (g + 1) * HEAD_SIZE] = done.T.astype(jnp.bfloat16)


def merge(own, got, m, l, m_got, l_got):
    all_heads, _, half = own.shape
    heads = all_heads // QUERY_GROUP
    part = pl.BlockSpec((QUERY_GROUP, HEAD_SIZE, half), lambda h: (h, 0, 0))
    stat = pl.BlockSpec((QUERY_GROUP, half), lambda h: (h, 0))
    return pl.pallas_call(
        merge_kernel,
        grid=(heads,),
        in_specs=[part, part, stat, stat, stat, stat],
        out_specs=pl.BlockSpec((1, half, QUERY_GROUP * HEAD_SIZE), lambda h: (0, 0, h)),
        out_shape=jax.ShapeDtypeStruct((1, half, all_heads * HEAD_SIZE), jnp.bfloat16),
        name="merge_halves",
    )(own, got, m, l, m_got, l_got)


def on_device(
    groups,
    n_ctx,
    stretch_query,
    prefix_keyvals,
    stretch_key_values,
    stretch_start,
    decode_query,
    draft_key_values,
    decode_cache,
    cache_lengths,
    page_rows,
):
    me = lax.axis_index("ctx")
    where = lax.axis_index("group") * n_ctx + me
    other = me + 1 - 2 * (me % 2)
    swap = [(i, i ^ 1) for i in range(n_ctx)]
    lines = n_ctx // 2
    heads = stretch_key_values.shape[3] // HEAD_SIZE
    stretch_rows = stretch_query.shape[1]
    shard_keys = prefix_keyvals.shape[2]

    page_count = groups * n_ctx
    even_pairs = [(n, (n + page_count // 2) % page_count) for n in range(0, page_count, 2)]
    odd_pairs = []
    for n in range(1, page_count, 2):
        g, c = divmod(n, n_ctx)
        odd_pairs.append(
            (n, (n + 1) % page_count if n % 4 == 1 else g * n_ctx + (c + n_ctx // 2) % n_ctx)
        )
    partner = lax.ppermute(stretch_query[0], "ctx", swap)
    page_own = stretch_key_values[0]
    even = lax.ppermute(page_own, ("group", "ctx"), even_pairs)
    odd = lax.ppermute(page_own, ("group", "ctx"), odd_pairs)
    shifts = []
    for s in range(1, lines // 2 + 1):
        shifts.append(s)
        if lines - s != s:
            shifts.append(lines - s)
    arrived = {}
    for s in shifts:
        ring = [(i, (i + 2 * s) % n_ctx) for i in range(n_ctx)]
        arrived[s] = (
            lax.ppermute(prefix_keyvals, "ctx", ring),
            lax.ppermute(stretch_key_values, "ctx", ring),
        )

    row_count, steps = decode_query.shape[:2]
    even_from = [-1] * page_count
    odd_from = [-1] * page_count
    for n, m in even_pairs:
        even_from[m] = n
    for n, m in odd_pairs:
        odd_from[m] = n

    def local_row(table):
        page = jnp.asarray(table, jnp.int32)[where]
        row = page_rows[jnp.maximum(page, 0)] - where * row_count
        return jnp.where(page >= 0, row, -1)

    decode_info = jnp.concatenate(
        [cache_lengths, jnp.stack([local_row(even_from), local_row(odd_from)])]
    ).astype(jnp.int32)
    decode_heads = (
        decode_query.reshape(row_count, steps, heads, QUERY_GROUP, HEAD_SIZE)
        .transpose(0, 2, 3, 1, 4)
        .reshape(row_count, heads, QUERY_GROUP * steps, HEAD_SIZE)
    )
    pad = -(-steps // 16) * 16
    draft = jnp.pad(draft_key_values, ((0, 0), (0, 0), (0, pad - steps), (0, 0)))
    decoded = decode(decode_info, decode_heads, decode_cache, draft, even, odd, steps)
    decode_out = (
        decoded.reshape(row_count, heads, QUERY_GROUP, steps, HEAD_SIZE)
        .transpose(0, 3, 1, 2, 4)
        .reshape(row_count, steps, heads * QUERY_GROUP * HEAD_SIZE)
    )

    queries = jnp.concatenate([stretch_query[0], partner], axis=0)

    def info_of(source):
        return jnp.stack([stretch_start[0], source * shard_keys, source, me, other]).astype(
            jnp.int32
        )

    state = stage(info_of(me), queries, prefix_keyvals, stretch_key_values, None, False)
    for s in shifts:
        source = (me + n_ctx - 2 * s) % n_ctx
        prefix, stretch = arrived[s]
        state = stage(info_of(source), queries, prefix, stretch, state, s == shifts[-1])
    m, l, own, send = state
    half = stretch_rows
    got = lax.ppermute(send, "ctx", swap)
    stats = lax.ppermute(jnp.stack([m[:, half:], l[:, half:]]), "ctx", swap)
    prefill_out = merge(own, got, m[:, :half], l[:, :half], stats[0], stats[1])
    return (prefill_out, decode_out)


def solution(mesh):
    return jax.shard_map(
        functools.partial(on_device, mesh.shape["group"], mesh.shape["ctx"]),
        mesh=mesh,
        in_specs=(
            P("group", "ctx", "tp"),
            P("group", None, "ctx", "tp"),
            P("group", None, "ctx", "tp"),
            P("group"),
            P(("group", "ctx"), None, "tp"),
            P(None, ("group", "ctx"), None, "tp"),
            P(None, ("group", "ctx"), None, "tp"),
            P(("group", "ctx")),
            P(),
        ),
        out_specs=(P("group", "ctx", "tp"), P(("group", "ctx"), None, "tp")),
        check_vma=False,
    )
```
